32 devices in a mesh: grp: 2 (over x), lat: 16 (over z, y, core).
Axes of the slice: x: 2, y: 2, z: 4, core: 2. Of those that a mesh axis runs over, the one named last changes fastest.
Arguments:
- acts: bfloat16 [128, 2, 2048], P(('grp', 'lat')), parts along dimension 0, may hold values from -6 to 6
- enc_weight: bfloat16 [4, 2048, 4096], P('grp', None, 'lat'), parts along dimension 0, may hold values from -0.09375 to 0.09375
- enc_bias: float32 [8192], P(('grp', 'lat')), parts along dimension 0, may hold values from -3 to 3
- dec_weight: bfloat16 [4096, 4, 2048], P('lat', 'grp'), parts along dimension 1, may hold values from -0.125 to 0.125
- dec_bias: float32 [4, 2048], P('grp'), parts along dimension 0, may hold values from -5 to 5
Outputs:
- residual: bfloat16 [128, 2, 2048], P(('grp', 'lat')), parts along dimension 0
- grad_enc: bfloat16 [4, 2048, 4096], P('grp', None, 'lat'), parts along dimension 0
- grad_enc_bias: float32 [8192], P(('grp', 'lat')), parts along dimension 0
- grad_dec: bfloat16 [4096, 4, 2048], P('lat', 'grp'), parts along dimension 1
- grad_dec_bias: float32 [4, 2048], P('grp'), parts along dimension 0
The draws below stay inside these ranges and needn't reach their ends.
There are 2 independent parts, one for each index of `grp`. The reference program is written for one: setup_inputs(seed, part) draws one part's arguments, and reference() takes and returns one part's arrays. A program takes and returns all parts, laid end to end along the dimension named above; each array names one. Nothing has to cross between parts.
All inputs are finite; a program needn't handle non-finite values.
Results may differ from the reference program's by a relative error of at most 0.015.
Values may be sent and summed in bfloat16 or wider, within the bound.
A program may use at most 128 MiB of HBM per device.

```python
import jax
import jax.numpy as jnp
from jax import lax

L = 2
D = 2048
FEATS = 4096
TOKENS = 64


def block_levels(own_key, shape, pieces, low, largest):
    loudness = 1.0
    for dim, blocks in pieces:
        draws = jax.random.uniform(jax.random.fold_in(jax.random.fold_in(own_key, 6), dim), (blocks,), jnp.float32, low / len(pieces), largest / len(pieces))
        loudness = loudness * jnp.repeat(jnp.exp(draws), shape[dim] // blocks).reshape((-1,) + (1,) * (len(shape) - 1 - dim))
    return loudness


def noise(key, extent, deviation, limit, split=(), kind=jnp.bfloat16):
    factor_of = block_levels(key, extent, split, -0.22, 0.18) if split else 1.0
    values = jax.random.normal(key, extent, jnp.float32) * deviation * factor_of
    return jnp.minimum(jnp.maximum(values, -limit), limit).astype(kind)


def setup_inputs(seed: int = 0, part: int = 0) -> dict:
    streams_of = jax.random.split(jax.random.key(seed), 6)
    part_splits = jax.random.split(jax.random.fold_in(streams_of[5], part), 6)
    return {
        "acts": noise(part_splits[0], (TOKENS, L, D), 1.0, 6.0, ((0, 16),)),
        "enc_weight": noise(part_splits[1], (L, D, FEATS), (L * D) ** -0.5, 0.09375, ((2, 16),)),
        "enc_bias": noise(part_splits[2], (FEATS,), 0.5, 3.0, ((0, 16),), jnp.float32),
        "dec_weight": noise(part_splits[3], (FEATS, L, D), D ** -0.5, 0.125, ((0, 16),)),
        "dec_bias": noise(part_splits[4], (L, D), 1.0, 5.0, (), jnp.float32),
    }


sparsity_weight = 2.0

def reference(acts, enc_weight, enc_bias, dec_weight, dec_bias):
    flat_rows = acts.reshape(TOKENS, L * D)
    flat_enc = enc_weight.reshape(L * D, FEATS)
    flat_dec = dec_weight.reshape(FEATS, L * D)
    before = jnp.dot(flat_rows, flat_enc, preferred_element_type=jnp.float32) + enc_bias
    active = jnp.maximum(before, 0.0).astype(jnp.bfloat16)
    rebuilt = jnp.dot(active, flat_dec, preferred_element_type=jnp.float32) + dec_bias.reshape(L * D)
    residual = (rebuilt - flat_rows.astype(jnp.float32)).astype(jnp.bfloat16)
    factor = 2.0 / TOKENS
    dec_wide = dec_weight.astype(jnp.float32)
    row_sq = lax.optimization_barrier(jnp.sum(dec_wide * dec_wide, axis=2))
    inv_norm = lax.rsqrt(row_sq + 1.0)
    dec_norm = lax.optimization_barrier(jnp.sum(jnp.sqrt(row_sq + 1.0), axis=1))
    backward = jnp.dot(residual, flat_dec.T, preferred_element_type=jnp.float32)
    grad_act = factor * backward + sparsity_weight / TOKENS * dec_norm
    grad_before = jnp.where(before > 0.0, grad_act, 0.0).astype(jnp.bfloat16)
    grad_enc = jnp.dot(flat_rows.T, grad_before, preferred_element_type=jnp.float32).astype(jnp.bfloat16).reshape(L, D, FEATS)
    grad_enc_bias = lax.optimization_barrier(jnp.sum(grad_before.astype(jnp.float32), axis=0))
    act_sum = lax.optimization_barrier(jnp.sum(active.astype(jnp.float32), axis=0))
    products = jnp.dot(active.T, residual, preferred_element_type=jnp.float32).reshape(FEATS, L, D)
    grad_dec = (factor * products + sparsity_weight / TOKENS * act_sum[:, None, None] * dec_wide * inv_norm[:, :, None]).astype(jnp.bfloat16)
    grad_dec_bias = (factor * lax.optimization_barrier(jnp.sum(residual.astype(jnp.float32), axis=0))).reshape(L, D)
    return (residual.reshape(TOKENS, L, D), grad_enc, grad_enc_bias, grad_dec, grad_dec_bias)
```

```python
import functools

import jax
import jax.numpy as jnp
from jax import lax
from jax.experimental import pallas as pl
from jax.experimental.pallas import tpu as pltpu
from jax.sharding import PartitionSpec as P

sparsity_weight = 2.0
f32, bf16 = jnp.float32, jnp.bfloat16


def dot(a, b, ca=1, cb=0):
    return lax.dot_general(a, b, (((ca,), (cb,)), ((), ())), preferred_element_type=f32)


def pair_expander(lat_dev, layers):
    row = lax.broadcasted_iota(jnp.int32, (lat_dev, lat_dev * layers), 0)
    col = lax.broadcasted_iota(jnp.int32, (lat_dev, lat_dev * layers), 1)
    return jnp.where(col // layers == row, 1.0, 0.0).astype(bf16)


def layer_major(rows, layers):
    size = rows * layers
    row = lax.broadcasted_iota(jnp.int32, (size, size), 0)
    col = lax.broadcasted_iota(jnp.int32, (size, size), 1)
    return jnp.where(row % rows * layers + row // rows == col, 1.0, 0.0).astype(bf16)


def spread_active(active, layers):
    rows, lat_dev = active.shape
    wide = dot(active, pair_expander(lat_dev, layers))
    layer = lax.broadcasted_iota(jnp.int32, wide.shape, 1) % layers
    parts = [jnp.where(layer == l, wide, 0.0).astype(bf16) for l in range(layers)]
    return jnp.concatenate(parts, axis=0)


def gather_kernel_body(n, src, buf, own_block, sems, me, send_to):
    chips = n // 2
    chip, core = me // 2, me % 2
    partner = me + 1 - 2 * core
    send, recv, fsend, frecv = sems

    def put(src_ref, index, ssem, rsem, dev):
        return pltpu.make_async_remote_copy(
            src_ref=src_ref, dst_ref=buf.at[index], send_sem=ssem, recv_sem=rsem,
            device_id={"lat": dev}, device_id_type=pl.DeviceIdType.MESH)

    first = []
    for q in range(1, chips):
        dev = lax.rem(chip + q, chips) * 2 + core
        c = put(src, me, send.at[q], recv.at[q], dev)
        c.start()
        first.append(c)
    second = [put(src, me, fsend.at[0], frecv.at[0], partner)]
    second[0].start()
    own_block()
    for q in range(1, chips):
        first[q - 1].wait_recv()
        origin = lax.rem(chip - q + chips, chips) * 2 + core
        c = put(buf.at[origin], origin, fsend.at[q], frecv.at[q], partner)
        c.start()
        second.append(c)
    for c in second:
        c.wait_recv()
    return first + second


def forward_kernel(n, acts, enc_hbm, bias, dec_hbm, dbias,
                   xl_out, rl_out, own_out, before_out, inv_out, norm_out,
                   enc, dec, w2, xbuf, rbuf, wide, rsrc, pair_out, pair_in, sum_out, sum_in,
                   local_sem, ag_sem, rg_sem, pair_sem, sum_sem):
    me = lax.axis_index("lat")
    chips = n // 2
    chip, core = me // 2, me % 2
    partner = me + 1 - 2 * core
    tok_dev, layers, width = acts.shape
    lat_dev = dec.shape[0]
    rows = n * tok_dev
    block = tok_dev * layers

    enc_copy = pltpu.make_async_copy(enc_hbm, enc, local_sem.at[0])
    dec_copy = pltpu.make_async_copy(dec_hbm, dec, local_sem.at[1])
    enc_copy.start()
    dec_copy.start()
    barrier = pltpu.get_barrier_semaphore()
    for q in range(1, chips):
        dev = lax.rem(chip + q, chips) * 2 + core
        pl.semaphore_signal(barrier, inc=1, device_id={"lat": dev}, device_id_type=pl.DeviceIdType.MESH)
    pl.semaphore_signal(barrier, inc=1, device_id={"lat": partner}, device_id_type=pl.DeviceIdType.MESH)
    pl.semaphore_wait(barrier, chips)

    def weight_work():
        xbuf[me] = acts[...]
        dec_copy.wait()
        square = jnp.zeros((lat_dev * layers, 128), f32)
        for c in range(0, width, 512):
            piece = dec[:, :, c:c + 512].reshape(lat_dev * layers, 512)
            w2[:, c:c + 512] = piece
            p = piece.astype(f32)
            p = p * p
            for k in range(4):
                square = square + p[:, k * 128:(k + 1) * 128]
        total = jnp.sum(square, axis=1, keepdims=True) + 1.0
        inv_out[...] = lax.rsqrt(total)
        norm = jnp.broadcast_to(jnp.sqrt(total), (lat_dev * layers, 128))
        norm_out[...] = jnp.transpose(norm)[:8, :]
        enc_copy.wait()

    started = gather_kernel_body(n, acts, xbuf, weight_work, [ag_sem.at[i] for i in range(4)], me, None)

    order_rows = layer_major(rows, layers)
    before = bias[...].reshape(1, lat_dev)
    for c in range(0, width, 512):
        piece = dot(order_rows, xbuf[:, :, :, c:c + 512].reshape(rows * layers, 512)).astype(bf16)
        xl_out[:, c:c + 512] = piece
        for l in range(layers):
            before = before + dot(piece[l * rows:(l + 1) * rows, :], enc[l, c:c + 512, :])
    before_out[...] = before
    active = jnp.maximum(before, 0.0).astype(bf16)
    spread = dot(order_rows, spread_active(active, layers), 0, 0).astype(bf16)
    for c in range(0, width, 512):
        wide[:, c:c + 512] = dot(spread, w2[:, c:c + 512])

    def chunk(dev):
        return wide[pl.ds(pl.multiple_of(dev * block, block), block), :]

    order = list(range(1, chips)) + [0]
    pairs = {}
    for q in order:
        k = lax.rem(chip + q, chips)
        pair_out[q] = chunk(k * 2 + 1 - core).astype(bf16)
        c = pltpu.make_async_remote_copy(
            src_ref=pair_out.at[q], dst_ref=pair_in.at[q], send_sem=pair_sem.at[0, q], recv_sem=pair_sem.at[1, q],
            device_id={"lat": partner}, device_id_type=pl.DeviceIdType.MESH)
        c.start()
        pairs[q] = c
    sums = []
    for q in order:
        k = lax.rem(chip + q, chips)
        pairs[q].wait_recv()
        both = chunk(k * 2 + core) + pair_in[q].astype(f32)
        if q == 0:
            total = both
        else:
            sum_out[q] = both.astype(bf16)
            c = pltpu.make_async_remote_copy(
                src_ref=sum_out.at[q], dst_ref=sum_in.at[q], send_sem=sum_sem.at[0, q], recv_sem=sum_sem.at[1, q],
                device_id={"lat": k * 2 + core}, device_id_type=pl.DeviceIdType.MESH)
            c.start()
            sums.append(c)
    layer = lax.broadcasted_iota(jnp.int32, (block, width), 0) % layers
    shift = jnp.zeros((block, width), f32)
    for l in range(layers):
        shift = jnp.where(layer == l, dbias[l:l + 1, :], shift)
    total = total + shift - acts[...].reshape(block, width).astype(f32)
    for q in range(1, chips):
        sums[q - 1].wait_recv()
        total = total + sum_in[q].astype(f32)
    residual = total.astype(bf16)
    rsrc[...] = residual
    own_out[...] = residual

    def own_residual():
        rbuf[me] = residual

    started += gather_kernel_body(n, rsrc, rbuf, own_residual, [rg_sem.at[i] for i in range(4)], me, None)
    for c in range(0, width, 512):
        piece = rbuf[:, :, c:c + 512].astype(f32).reshape(rows * layers, 512).astype(bf16)
        rl_out[:, c:c + 512] = dot(order_rows, piece).astype(bf16)
    for c in started + list(pairs.values()) + sums:
        c.wait_send()


def backward_kernel(xl, rl, own, before, inv, norm, dec, residual, genc, gencb, gdec, gdecb):
    layers, width, lat_dev = genc.shape
    rows = before.shape[0]
    factor = 2.0 / rows
    step = 512
    residual[...] = own[...].reshape(residual.shape)
    back = jnp.zeros((rows * layers, lat_dev * layers), f32)
    for c in range(0, width, step):
        back = back + dot(rl[:, c:c + step], dec[:, :, c:c + step].reshape(lat_dev * layers, step), 1, 1)
    layer = lax.broadcasted_iota(jnp.int32, (rows, lat_dev * layers), 1) % layers
    value = jnp.zeros((rows, lat_dev * layers), f32)
    for l in range(layers):
        value = jnp.where(layer == l, back[l * rows:(l + 1) * rows, :], value)
    value = factor * value + (sparsity_weight / rows) * norm[0:1, :]
    high = value.astype(bf16)
    low = (value - high.astype(f32)).astype(bf16)
    expand = pair_expander(lat_dev, layers)
    grad_act = dot(high, expand, 1, 1) + dot(low, expand, 1, 1)
    pre = before[...]
    grad_before = jnp.where(pre > 0.0, grad_act, 0.0).astype(bf16)
    gencb[...] = jnp.sum(grad_before.astype(f32), axis=0, keepdims=True)
    for l in range(layers):
        for c in range(0, width, step):
            genc[l, c:c + step, :] = dot(xl[l * rows:(l + 1) * rows, c:c + step], grad_before, 0, 0).astype(bf16)
    spread = spread_active(jnp.maximum(pre, 0.0).astype(bf16), layers)
    act_sum = dot(spread, jnp.ones((rows * layers, 128), bf16), 0, 0)[:, :1]
    scale = (sparsity_weight / rows) * act_sum * inv[...]
    for c in range(0, width, step):
        wide = dec[:, :, c:c + step].reshape(lat_dev * layers, step).astype(f32)
        out = factor * dot(spread, rl[:, c:c + step], 0, 0) + scale * wide
        gdec[:, :, c:c + step] = out.astype(bf16).reshape(lat_dev, layers, step)
    for l in range(layers):
        gdecb[l:l + 1, :] = factor * jnp.sum(rl[l * rows:(l + 1) * rows, :].astype(f32), axis=0, keepdims=True)


def body(n, acts, enc_weight, enc_bias, dec_weight, dec_bias):
    tok_dev, layers, width = acts.shape
    lat_dev = enc_weight.shape[2]
    rows, block, chips = n * tok_dev, tok_dev * layers, n // 2
    vmem = pl.BlockSpec(memory_space=pltpu.VMEM)
    hbm = pl.BlockSpec(memory_space=pl.ANY)
    shape = jax.ShapeDtypeStruct
    dma = pltpu.SemaphoreType.DMA
    xl, rl, own, before, inv, norm = pl.pallas_call(
        functools.partial(forward_kernel, n),
        out_shape=(
            shape((rows * layers, width), bf16),
            shape((rows * layers, width), bf16),
            shape((block, width), bf16),
            shape((rows, lat_dev), f32),
            shape((lat_dev * layers, 1), f32),
            shape((8, lat_dev * layers), f32),
        ),
        in_specs=[vmem, hbm, vmem, hbm, vmem],
        out_specs=(vmem,) * 6,
        scratch_shapes=[
            pltpu.VMEM(enc_weight.shape, bf16),
            pltpu.VMEM(dec_weight.shape, bf16),
            pltpu.VMEM((lat_dev * layers, width), bf16),
            pltpu.VMEM((n, tok_dev, layers, width), bf16),
            pltpu.VMEM((n, block, width), bf16),
            pltpu.VMEM((rows * layers, width), f32),
            pltpu.VMEM((block, width), bf16),
            pltpu.VMEM((chips, block, width), bf16),
            pltpu.VMEM((chips, block, width), bf16),
            pltpu.VMEM((chips, block, width), bf16),
            pltpu.VMEM((chips, block, width), bf16),
            dma((2,)),
            dma((4, chips)),
            dma((4, chips)),
            dma((2, chips)),
            dma((2, chips)),
        ],
        compiler_params=pltpu.CompilerParams(
            collective_id=0, has_side_effects=True, vmem_limit_bytes=56 * 1024 * 1024),
        name="forward",
    )(acts, enc_weight, enc_bias.reshape(1, lat_dev), dec_weight, dec_bias)
    residual, genc, gencb, gdec, gdecb = pl.pallas_call(
        backward_kernel,
        out_shape=(
            shape(acts.shape, bf16),
            shape(enc_weight.shape, bf16),
            shape((1, lat_dev), f32),
            shape(dec_weight.shape, bf16),
            shape(dec_bias.shape, f32),
        ),
        in_specs=[vmem] * 7,
        out_specs=(vmem,) * 5,
        compiler_params=pltpu.CompilerParams(vmem_limit_bytes=56 * 1024 * 1024),
        name="backward",
    )(xl, rl, own, before, inv, norm, dec_weight)
    return residual, genc, gencb.reshape(lat_dev), gdec, gdecb


def solution(mesh):
    specs = (
        P(("grp", "lat"), None, None),
        P("grp", None, "lat"),
        P(("grp", "lat")),
        P("lat", "grp", None),
        P("grp", None),
    )
    return jax.shard_map(
        functools.partial(body, mesh.shape["lat"]),
        mesh=mesh, in_specs=specs, out_specs=specs, check_vma=False,
    )
```

```python
import functools

import jax
import jax.numpy as jnp
from jax import lax
from jax.experimental import pallas as pl
from jax.experimental.pallas import tpu as pltpu
from jax.sharding import PartitionSpec as P

sparsity_weight = 2.0
f32, bf16 = jnp.float32, jnp.bfloat16


def dot(a, b, ca=1, cb=0):
    return lax.dot_general(a, b, (((ca,), (cb,)), ((), ())), preferred_element_type=f32)


def pair_expander(lat_dev, layers):
    row = lax.broadcasted_iota(jnp.int32, (lat_dev, lat_dev * layers), 0)
    col = lax.broadcasted_iota(jnp.int32, (lat_dev, lat_dev * layers), 1)
    return jnp.where(col // layers == row, 1.0, 0.0).astype(bf16)


def layer_major(rows, layers):
    size = rows * layers
    row = lax.broadcasted_iota(jnp.int32, (size, size), 0)
    col = lax.broadcasted_iota(jnp.int32, (size, size), 1)
    return jnp.where(row % rows * layers + row // rows == col, 1.0, 0.0).astype(bf16)


def spread_active(active, layers):
    rows, lat_dev = active.shape
    wide = dot(active, pair_expander(lat_dev, layers))
    layer = lax.broadcasted_iota(jnp.int32, wide.shape, 1) % layers
    parts = [jnp.where(layer == l, wide, 0.0).astype(bf16) for l in range(layers)]
    return jnp.concatenate(parts, axis=0)


def grid_of(n):
    chips = n // 2
    inner = max(k for k in range(1, chips + 1) if chips % k == 0 and k * k <= chips)
    return chips // inner, inner


def gather_blocks(n, src, buf, own_block, outer_sem, inner_sem, core_sem):
    outer, inner = grid_of(n)
    me = lax.axis_index("lat")
    core, y, z = me % 2, me // 2 % inner, me // (2 * inner)
    partner = me + 1 - 2 * core
    started = []

    def put(src_ref, index, sems, slot, dev):
        c = pltpu.make_async_remote_copy(
            src_ref=src_ref, dst_ref=buf.at[index],
            send_sem=sems.at[(0,) + slot], recv_sem=sems.at[(1,) + slot],
            device_id={"lat": dev}, device_id_type=pl.DeviceIdType.MESH)
        c.start()
        started.append(c)
        return c

    along_outer, along_inner, to_partner = {}, {}, []
    for q in range(1, outer):
        dev = (lax.rem(z + q, outer) * inner + y) * 2 + core
        along_outer[q] = put(src, me, outer_sem, (q,), dev)
    for q in range(outer):
        origin = (lax.rem(z - q + outer, outer) * inner + y) * 2 + core
        if q:
            along_outer[q].wait_recv()
        block = buf.at[origin] if q else src
        for r in range(1, inner):
            dev = (z * inner + lax.rem(y + r, inner)) * 2 + core
            along_inner[q, r] = put(block, origin, inner_sem, (q, r), dev)
        to_partner.append(put(block, origin, core_sem, (q, 0), partner))
        if q == 0:
            own_block()
    for q in range(outer):
        for r in range(1, inner):
            origin = (lax.rem(z - q + outer, outer) * inner + lax.rem(y - r + inner, inner)) * 2 + core
            along_inner[q, r].wait_recv()
            to_partner.append(put(buf.at[origin], origin, core_sem, (q, r), partner))
    for c in to_partner:
        c.wait_recv()
    return started


def forward_kernel(n, acts, enc_hbm, bias, dec_hbm, dbias,
                   xl_out, rl_out, own_out, before_out, inv_out, norm_out,
                   enc, dec, w2, xbuf, rbuf, wide, rsrc, pair_out, pair_in, sum_out, sum_in,
                   local_sem, pair_sem, sum_sem, *gather_sems):
    ag_sems, rg_sems = gather_sems[:3], gather_sems[3:]
    me = lax.axis_index("lat")
    chips = n // 2
    chip, core = me // 2, me % 2
    partner = me + 1 - 2 * core
    tok_dev, layers, width = acts.shape
    lat_dev = dec.shape[0]
    rows = n * tok_dev
    block = tok_dev * layers

    enc_copy = pltpu.make_async_copy(enc_hbm, enc, local_sem.at[0])
    dec_copy = pltpu.make_async_copy(dec_hbm, dec, local_sem.at[1])
    enc_copy.start()
    dec_copy.start()
    barrier = pltpu.get_barrier_semaphore()
    for q in range(1, chips):
        dev = lax.rem(chip + q, chips) * 2 + core
        pl.semaphore_signal(barrier, inc=1, device_id={"lat": dev}, device_id_type=pl.DeviceIdType.MESH)
    pl.semaphore_signal(barrier, inc=1, device_id={"lat": partner}, device_id_type=pl.DeviceIdType.MESH)
    pl.semaphore_wait(barrier, chips)

    def weight_work():
        xbuf[me] = acts[...]
        dec_copy.wait()
        square = jnp.zeros((lat_dev * layers, 128), f32)
        for c in range(0, width, 512):
            piece = dec[:, :, c:c + 512].reshape(lat_dev * layers, 512)
            w2[:, c:c + 512] = piece
            p = piece.astype(f32)
            p = p * p
            for k in range(4):
                square = square + p[:, k * 128:(k + 1) * 128]
        total = jnp.sum(square, axis=1, keepdims=True) + 1.0
        inv_out[...] = lax.rsqrt(total)
        norm = jnp.broadcast_to(jnp.sqrt(total), (lat_dev * layers, 128))
        norm_out[...] = jnp.transpose(norm)[:8, :]
        enc_copy.wait()

    started = gather_blocks(n, acts, xbuf, weight_work, *ag_sems)

    order_rows = layer_major(rows, layers)
    before = bias[...].reshape(1, lat_dev)
    for c in range(0, width, 512):
        piece = dot(order_rows, xbuf[:, :, :, c:c + 512].reshape(rows * layers, 512)).astype(bf16)
        xl_out[:, c:c + 512] = piece
        for l in range(layers):
            before = before + dot(piece[l * rows:(l + 1) * rows, :], enc[l, c:c + 512, :])
    before_out[...] = before
    active = jnp.maximum(before, 0.0).astype(bf16)
    spread = dot(order_rows, spread_active(active, layers), 0, 0).astype(bf16)
    for c in range(0, width, 512):
        wide[:, c:c + 512] = dot(spread, w2[:, c:c + 512])

    def chunk(dev):
        return wide[pl.ds(pl.multiple_of(dev * block, block), block), :]

    order = list(range(1, chips)) + [0]
    pairs = {}
    for q in order:
        k = lax.rem(chip + q, chips)
        pair_out[q] = chunk(k * 2 + 1 - core).astype(bf16)
        c = pltpu.make_async_remote_copy(
            src_ref=pair_out.at[q], dst_ref=pair_in.at[q], send_sem=pair_sem.at[0, q], recv_sem=pair_sem.at[1, q],
            device_id={"lat": partner}, device_id_type=pl.DeviceIdType.MESH)
        c.start()
        pairs[q] = c
    sums = []
    for q in order:
        k = lax.rem(chip + q, chips)
        pairs[q].wait_recv()
        both = chunk(k * 2 + core) + pair_in[q].astype(f32)
        if q == 0:
            total = both
        else:
            sum_out[q] = both.astype(bf16)
            c = pltpu.make_async_remote_copy(
                src_ref=sum_out.at[q], dst_ref=sum_in.at[q], send_sem=sum_sem.at[0, q], recv_sem=sum_sem.at[1, q],
                device_id={"lat": k * 2 + core}, device_id_type=pl.DeviceIdType.MESH)
            c.start()
            sums.append(c)
    layer = lax.broadcasted_iota(jnp.int32, (block, width), 0) % layers
    shift = jnp.zeros((block, width), f32)
    for l in range(layers):
        shift = jnp.where(layer == l, dbias[l:l + 1, :], shift)
    total = total + shift - acts[...].reshape(block, width).astype(f32)
    for q in range(1, chips):
        sums[q - 1].wait_recv()
        total = total + sum_in[q].astype(f32)
    residual = total.astype(bf16)
    rsrc[...] = residual
    own_out[...] = residual

    def own_residual():
        rbuf[me] = residual

    started += gather_blocks(n, rsrc, rbuf, own_residual, *rg_sems)
    for c in range(0, width, 512):
        piece = rbuf[:, :, c:c + 512].astype(f32).reshape(rows * layers, 512).astype(bf16)
        rl_out[:, c:c + 512] = dot(order_rows, piece).astype(bf16)
    for c in started + list(pairs.values()) + sums:
        c.wait_send()


def backward_kernel(xl, rl, own, before, inv, norm, dec_hbm, residual, genc_hbm, gencb, gdec_hbm, gdecb,
                    dec, genc, gdec, in_sem, dec_sem, enc_sem):
    layers, width, lat_dev = genc.shape
    rows = before.shape[0]
    factor = 2.0 / rows
    pieces = dec_sem.shape[0]
    step = width // pieces
    cuts = [slice(i * step, (i + 1) * step) for i in range(pieces)]
    loads = [pltpu.make_async_copy(dec_hbm.at[:, :, c], dec.at[:, :, c], in_sem.at[i]) for i, c in enumerate(cuts)]
    for c in loads:
        c.start()
    residual[...] = own[...].reshape(residual.shape)
    for l in range(layers):
        gdecb[l:l + 1, :] = factor * jnp.sum(rl[l * rows:(l + 1) * rows, :].astype(f32), axis=0, keepdims=True)
    pre = before[...]
    spread = spread_active(jnp.maximum(pre, 0.0).astype(bf16), layers)
    act_sum = dot(spread, jnp.ones((rows * layers, 128), bf16), 0, 0)[:, :1]
    scale = (sparsity_weight / rows) * act_sum * inv[...]
    spread_t = jnp.transpose(spread)
    back = jnp.zeros((rows * layers, lat_dev * layers), f32)
    stores = []
    for i, c in enumerate(cuts):
        loads[i].wait()
        piece = dec[:, :, c].reshape(lat_dev * layers, step)
        back = back + dot(rl[:, c], piece, 1, 1)
        out = factor * dot(spread_t, rl[:, c]) + scale * piece.astype(f32)
        gdec[:, :, c] = out.astype(bf16).reshape(lat_dev, layers, step)
        stores.append(pltpu.make_async_copy(gdec.at[:, :, c], gdec_hbm.at[:, :, c], dec_sem.at[i]))
        stores[-1].start()
    layer = lax.broadcasted_iota(jnp.int32, (rows, lat_dev * layers), 1) % layers
    value = jnp.zeros((rows, lat_dev * layers), f32)
    for l in range(layers):
        value = jnp.where(layer == l, back[l * rows:(l + 1) * rows, :], value)
    value = factor * value + (sparsity_weight / rows) * norm[0:1, :]
    high = value.astype(bf16)
    low = (value - high.astype(f32)).astype(bf16)
    expand = pair_expander(lat_dev, layers)
    grad_act = dot(high, expand, 1, 1) + dot(low, expand, 1, 1)
    grad_before = jnp.where(pre > 0.0, grad_act, 0.0).astype(bf16)
    gencb[...] = jnp.sum(grad_before.astype(f32), axis=0, keepdims=True)
    for l in range(layers):
        for i, c in enumerate(cuts):
            genc[l, c, :] = dot(xl[l * rows:(l + 1) * rows, c], grad_before, 0, 0).astype(bf16)
            stores.append(pltpu.make_async_copy(genc.at[l, c], genc_hbm.at[l, c], enc_sem.at[l, i]))
            stores[-1].start()
    for c in stores:
        c.wait()


def body(n, acts, enc_weight, enc_bias, dec_weight, dec_bias):
    tok_dev, layers, width = acts.shape
    lat_dev = enc_weight.shape[2]
    rows, block, chips = n * tok_dev, tok_dev * layers, n // 2
    outer, inner = grid_of(n)
    vmem = pl.BlockSpec(memory_space=pltpu.VMEM)
    hbm = pl.BlockSpec(memory_space=pl.ANY)
    shape = jax.ShapeDtypeStruct
    dma = pltpu.SemaphoreType.DMA
    xl, rl, own, before, inv, norm = pl.pallas_call(
        functools.partial(forward_kernel, n),
        out_shape=(
            shape((rows * layers, width), bf16),
            shape((rows * layers, width), bf16),
            shape((block, width), bf16),
            shape((rows, lat_dev), f32),
            shape((lat_dev * layers, 1), f32),
            shape((8, lat_dev * layers), f32),
        ),
        in_specs=[vmem, hbm, vmem, hbm, vmem],
        out_specs=(vmem,) * 6,
        scratch_shapes=[
            pltpu.VMEM(enc_weight.shape, bf16),
            pltpu.VMEM(dec_weight.shape, bf16),
            pltpu.VMEM((lat_dev * layers, width), bf16),
            pltpu.VMEM((n, tok_dev, layers, width), bf16),
            pltpu.VMEM((n, block, width), bf16),
            pltpu.VMEM((rows * layers, width), f32),
            pltpu.VMEM((block, width), bf16),
            pltpu.VMEM((chips, block, width), bf16),
            pltpu.VMEM((chips, block, width), bf16),
            pltpu.VMEM((chips, block, width), bf16),
            pltpu.VMEM((chips, block, width), bf16),
            dma((2,)),
            dma((2, chips)),
            dma((2, chips)),
        ] + [dma((2, outer)), dma((2, outer, inner)), dma((2, outer, inner))] * 2,
        compiler_params=pltpu.CompilerParams(
            collective_id=0, has_side_effects=True, vmem_limit_bytes=56 * 1024 * 1024),
        name="forward",
    )(acts, enc_weight, enc_bias.reshape(1, lat_dev), dec_weight, dec_bias)
    residual, genc, gencb, gdec, gdecb = pl.pallas_call(
        backward_kernel,
        out_shape=(
            shape(acts.shape, bf16),
            shape(enc_weight.shape, bf16),
            shape((1, lat_dev), f32),
            shape(dec_weight.shape, bf16),
            shape(dec_bias.shape, f32),
        ),
        in_specs=[vmem] * 6 + [hbm],
        out_specs=(vmem, hbm, vmem, hbm, vmem),
        scratch_shapes=[
            pltpu.VMEM(dec_weight.shape, bf16),
            pltpu.VMEM(enc_weight.shape, bf16),
            pltpu.VMEM(dec_weight.shape, bf16),
            dma((4,)),
            dma((4,)),
            dma((layers, 4)),
        ],
        compiler_params=pltpu.CompilerParams(vmem_limit_bytes=56 * 1024 * 1024),
        name="backward",
    )(xl, rl, own, before, inv, norm, dec_weight)
    return residual, genc, gencb.reshape(lat_dev), gdec, gdecb


def solution(mesh):
    specs = (
        P(("grp", "lat"), None, None),
        P("grp", None, "lat"),
        P(("grp", "lat")),
        P("lat", "grp", None),
        P("grp", None),
    )
    return jax.shard_map(
        functools.partial(body, mesh.shape["lat"]),
        mesh=mesh, in_specs=specs, out_specs=specs, check_vma=False,
    )
```

```python
import functools

import jax
import jax.numpy as jnp
from jax import lax
from jax.experimental import pallas as pl
from jax.experimental.pallas import tpu as pltpu
from jax.sharding import PartitionSpec as P

sparsity_weight = 2.0
f32, bf16 = jnp.float32, jnp.bfloat16


def dot(a, b, ca=1, cb=0):
    return lax.dot_general(a, b, (((ca,), (cb,)), ((), ())), preferred_element_type=f32)


def pair_expander(lat_dev, layers):
    row = lax.broadcasted_iota(jnp.int32, (lat_dev, lat_dev * layers), 0)
    col = lax.broadcasted_iota(jnp.int32, (lat_dev, lat_dev * layers), 1)
    return jnp.where(col // layers == row, 1.0, 0.0).astype(bf16)


def layer_major(rows, layers):
    size = rows * layers
    row = lax.broadcasted_iota(jnp.int32, (size, size), 0)
    col = lax.broadcasted_iota(jnp.int32, (size, size), 1)
    return jnp.where(row % rows * layers + row // rows == col, 1.0, 0.0).astype(bf16)


def spread_active(active, layers):
    rows, lat_dev = active.shape
    wide = dot(active, pair_expander(lat_dev, layers))
    layer = lax.broadcasted_iota(jnp.int32, wide.shape, 1) % layers
    parts = [jnp.where(layer == l, wide, 0.0).astype(bf16) for l in range(layers)]
    return jnp.concatenate(parts, axis=0)


def gather_kernel_body(n, src, buf, own_block, sems, me, send_to):
    chips = n // 2
    chip, core = me // 2, me % 2
    partner = me + 1 - 2 * core
    send, recv, fsend, frecv = sems

    def put(src_ref, index, ssem, rsem, dev):
        return pltpu.make_async_remote_copy(
            src_ref=src_ref, dst_ref=buf.at[index], send_sem=ssem, recv_sem=rsem,
            device_id={"lat": dev}, device_id_type=pl.DeviceIdType.MESH)

    first = []
    for q in range(1, chips):
        dev = lax.rem(chip + q, chips) * 2 + core
        c = put(src, me, send.at[q], recv.at[q], dev)
        c.start()
        first.append(c)
    second = [put(src, me, fsend.at[0], frecv.at[0], partner)]
    second[0].start()
    own_block()
    for q in range(1, chips):
        first[q - 1].wait_recv()
        origin = lax.rem(chip - q + chips, chips) * 2 + core
        c = put(buf.at[origin], origin, fsend.at[q], frecv.at[q], partner)
        c.start()
        second.append(c)
    for c in second:
        c.wait_recv()
    return first + second


def forward_kernel(n, acts, enc_hbm, bias, dec_hbm, dbias,
                   xl_out, rl_out, own_out, before_out, inv_out, norm_out,
                   enc, dec, w2, xbuf, rbuf, wide, rsrc, pair_out, pair_in, sum_out, sum_in,
                   local_sem, ag_sem, rg_sem, pair_sem, sum_sem):
    me = lax.axis_index("lat")
    chips = n // 2
    chip, core = me // 2, me % 2
    partner = me + 1 - 2 * core
    tok_dev, layers, width = acts.shape
    lat_dev = dec.shape[0]
    rows = n * tok_dev
    block = tok_dev * layers

    enc_copy = pltpu.make_async_copy(enc_hbm, enc, local_sem.at[0])
    dec_copy = pltpu.make_async_copy(dec_hbm, dec, local_sem.at[1])
    enc_copy.start()
    dec_copy.start()
    barrier = pltpu.get_barrier_semaphore()
    for q in range(1, chips):
        dev = lax.rem(chip + q, chips) * 2 + core
        pl.semaphore_signal(barrier, inc=1, device_id={"lat": dev}, device_id_type=pl.DeviceIdType.MESH)
    pl.semaphore_signal(barrier, inc=1, device_id={"lat": partner}, device_id_type=pl.DeviceIdType.MESH)
    pl.semaphore_wait(barrier, chips)

    def weight_work():
        xbuf[me] = acts[...]
        dec_copy.wait()
        square = jnp.zeros((lat_dev * layers, 128), f32)
        for c in range(0, width, 512):
            piece = dec[:, :, c:c + 512].reshape(lat_dev * layers, 512)
            w2[:, c:c + 512] = piece
            p = piece.astype(f32)
            p = p * p
            for k in range(4):
                square = square + p[:, k * 128:(k + 1) * 128]
        total = jnp.sum(square, axis=1, keepdims=True) + 1.0
        inv_out[...] = lax.rsqrt(total)
        norm = jnp.broadcast_to(jnp.sqrt(total), (lat_dev * layers, 128))
        norm_out[...] = jnp.transpose(norm)[:8, :]
        enc_copy.wait()

    started = gather_kernel_body(n, acts, xbuf, weight_work, [ag_sem.at[i] for i in range(4)], me, None)

    order_rows = layer_major(rows, layers)
    before = bias[...].reshape(1, lat_dev)
    for c in range(0, width, 512):
        piece = dot(order_rows, xbuf[:, :, :, c:c + 512].reshape(rows * layers, 512)).astype(bf16)
        xl_out[:, c:c + 512] = piece
        for l in range(layers):
            before = before + dot(piece[l * rows:(l + 1) * rows, :], enc[l, c:c + 512, :])
    before_out[...] = before
    active = jnp.maximum(before, 0.0).astype(bf16)
    spread = dot(order_rows, spread_active(active, layers), 0, 0).astype(bf16)
    for c in range(0, width, 512):
        wide[:, c:c + 512] = dot(spread, w2[:, c:c + 512])

    def chunk(dev):
        return wide[pl.ds(pl.multiple_of(dev * block, block), block), :]

    order = list(range(1, chips)) + [0]
    pairs = {}
    for q in order:
        k = lax.rem(chip + q, chips)
        pair_out[q] = chunk(k * 2 + 1 - core).astype(bf16)
        c = pltpu.make_async_remote_copy(
            src_ref=pair_out.at[q], dst_ref=pair_in.at[q], send_sem=pair_sem.at[0, q], recv_sem=pair_sem.at[1, q],
            device_id={"lat": partner}, device_id_type=pl.DeviceIdType.MESH)
        c.start()
        pairs[q] = c
    sums = []
    for q in order:
        k = lax.rem(chip + q, chips)
        pairs[q].wait_recv()
        both = chunk(k * 2 + core) + pair_in[q].astype(f32)
        if q == 0:
            total = both
        else:
            sum_out[q] = both.astype(bf16)
            c = pltpu.make_async_remote_copy(
                src_ref=sum_out.at[q], dst_ref=sum_in.at[q], send_sem=sum_sem.at[0, q], recv_sem=sum_sem.at[1, q],
                device_id={"lat": k * 2 + core}, device_id_type=pl.DeviceIdType.MESH)
            c.start()
            sums.append(c)
    layer = lax.broadcasted_iota(jnp.int32, (block, width), 0) % layers
    shift = jnp.zeros((block, width), f32)
    for l in range(layers):
        shift = jnp.where(layer == l, dbias[l:l + 1, :], shift)
    total = total + shift - acts[...].reshape(block, width).astype(f32)
    for q in range(1, chips):
        sums[q - 1].wait_recv()
        total = total + sum_in[q].astype(f32)
    residual = total.astype(bf16)
    rsrc[...] = residual
    own_out[...] = residual

    def own_residual():
        rbuf[me] = residual

    started += gather_kernel_body(n, rsrc, rbuf, own_residual, [rg_sem.at[i] for i in range(4)], me, None)
    for c in range(0, width, 512):
        piece = rbuf[:, :, c:c + 512].astype(f32).reshape(rows * layers, 512).astype(bf16)
        rl_out[:, c:c + 512] = dot(order_rows, piece).astype(bf16)
    for c in started + list(pairs.values()) + sums:
        c.wait_send()


def backward_kernel(xl, rl, own, before, inv, norm, dec, residual, genc_hbm, gencb, gdec_hbm, gdecb,
                    genc, gdec, out_sem):
    layers, width, lat_dev = genc.shape
    rows = before.shape[0]
    factor = 2.0 / rows
    step = 512
    pre = before[...]
    spread = spread_active(jnp.maximum(pre, 0.0).astype(bf16), layers)
    act_sum = dot(spread, jnp.ones((rows * layers, 128), bf16), 0, 0)[:, :1]
    scale = (sparsity_weight / rows) * act_sum * inv[...]
    for c in range(0, width, step):
        wide = dec[:, :, c:c + step].reshape(lat_dev * layers, step).astype(f32)
        out = factor * dot(spread, rl[:, c:c + step], 0, 0) + scale * wide
        gdec[:, :, c:c + step] = out.astype(bf16).reshape(lat_dev, layers, step)
    stores = [pltpu.make_async_copy(gdec, gdec_hbm, out_sem.at[layers])]
    stores[0].start()
    back = jnp.zeros((rows * layers, lat_dev * layers), f32)
    for c in range(0, width, step):
        back = back + dot(rl[:, c:c + step], dec[:, :, c:c + step].reshape(lat_dev * layers, step), 1, 1)
    layer = lax.broadcasted_iota(jnp.int32, (rows, lat_dev * layers), 1) % layers
    value = jnp.zeros((rows, lat_dev * layers), f32)
    for l in range(layers):
        value = jnp.where(layer == l, back[l * rows:(l + 1) * rows, :], value)
    value = factor * value + (sparsity_weight / rows) * norm[0:1, :]
    high = value.astype(bf16)
    low = (value - high.astype(f32)).astype(bf16)
    expand = pair_expander(lat_dev, layers)
    grad_act = dot(high, expand, 1, 1) + dot(low, expand, 1, 1)
    grad_before = jnp.where(pre > 0.0, grad_act, 0.0).astype(bf16)
    gencb[...] = jnp.sum(grad_before.astype(f32), axis=0, keepdims=True)
    for l in range(layers):
        for c in range(0, width, step):
            genc[l, c:c + step, :] = dot(xl[l * rows:(l + 1) * rows, c:c + step], grad_before, 0, 0).astype(bf16)
        stores.append(pltpu.make_async_copy(genc.at[l], genc_hbm.at[l], out_sem.at[l]))
        stores[-1].start()
    residual[...] = own[...].reshape(residual.shape)
    for l in range(layers):
        gdecb[l:l + 1, :] = factor * jnp.sum(rl[l * rows:(l + 1) * rows, :].astype(f32), axis=0, keepdims=True)
    for c in stores:
        c.wait()


def body(n, acts, enc_weight, enc_bias, dec_weight, dec_bias):
    tok_dev, layers, width = acts.shape
    lat_dev = enc_weight.shape[2]
    rows, block, chips = n * tok_dev, tok_dev * layers, n // 2
    vmem = pl.BlockSpec(memory_space=pltpu.VMEM)
    hbm = pl.BlockSpec(memory_space=pl.ANY)
    shape = jax.ShapeDtypeStruct
    dma = pltpu.SemaphoreType.DMA
    xl, rl, own, before, inv, norm = pl.pallas_call(
        functools.partial(forward_kernel, n),
        out_shape=(
            shape((rows * layers, width), bf16),
            shape((rows * layers, width), bf16),
            shape((block, width), bf16),
            shape((rows, lat_dev), f32),
            shape((lat_dev * layers, 1), f32),
            shape((8, lat_dev * layers), f32),
        ),
        in_specs=[vmem, hbm, vmem, hbm, vmem],
        out_specs=(vmem,) * 6,
        scratch_shapes=[
            pltpu.VMEM(enc_weight.shape, bf16),
            pltpu.VMEM(dec_weight.shape, bf16),
            pltpu.VMEM((lat_dev * layers, width), bf16),
            pltpu.VMEM((n, tok_dev, layers, width), bf16),
            pltpu.VMEM((n, block, width), bf16),
            pltpu.VMEM((rows * layers, width), f32),
            pltpu.VMEM((block, width), bf16),
            pltpu.VMEM((chips, block, width), bf16),
            pltpu.VMEM((chips, block, width), bf16),
            pltpu.VMEM((chips, block, width), bf16),
            pltpu.VMEM((chips, block, width), bf16),
            dma((2,)),
            dma((4, chips)),
            dma((4, chips)),
            dma((2, chips)),
            dma((2, chips)),
        ],
        compiler_params=pltpu.CompilerParams(
            collective_id=0, has_side_effects=True, vmem_limit_bytes=56 * 1024 * 1024),
        name="forward",
    )(acts, enc_weight, enc_bias.reshape(1, lat_dev), dec_weight, dec_bias)
    residual, genc, gencb, gdec, gdecb = pl.pallas_call(
        backward_kernel,
        out_shape=(
            shape(acts.shape, bf16),
            shape(enc_weight.shape, bf16),
            shape((1, lat_dev), f32),
            shape(dec_weight.shape, bf16),
            shape(dec_bias.shape, f32),
        ),
        in_specs=[vmem] * 7,
        out_specs=(vmem, hbm, vmem, hbm, vmem),
        scratch_shapes=[
            pltpu.VMEM(enc_weight.shape, bf16),
            pltpu.VMEM(dec_weight.shape, bf16),
            dma((layers + 1,)),
        ],
        compiler_params=pltpu.CompilerParams(vmem_limit_bytes=56 * 1024 * 1024),
        name="backward",
    )(xl, rl, own, before, inv, norm, dec_weight)
    return residual, genc, gencb.reshape(lat_dev), gdec, gdecb


def solution(mesh):
    specs = (
        P(("grp", "lat"), None, None),
        P("grp", None, "lat"),
        P(("grp", "lat")),
        P("lat", "grp", None),
        P("grp", None),
    )
    return jax.shard_map(
        functools.partial(body, mesh.shape["lat"]),
        mesh=mesh, in_specs=specs, out_specs=specs, check_vma=False,
    )
```

```python
import functools

import jax
import jax.numpy as jnp
from jax import lax
from jax.experimental import pallas as pl
from jax.experimental.pallas import tpu as pltpu
from jax.sharding import PartitionSpec as P

sparsity_weight = 2.0
f32, bf16 = jnp.float32, jnp.bfloat16


def dot(a, b, ca=1, cb=0):
    return lax.dot_general(a, b, (((ca,), (cb,)), ((), ())), preferred_element_type=f32)


def pair_expander(lat_dev, layers):
    row = lax.broadcasted_iota(jnp.int32, (lat_dev, lat_dev * layers), 0)
    col = lax.broadcasted_iota(jnp.int32, (lat_dev, lat_dev * layers), 1)
    return jnp.where(col // layers == row, 1.0, 0.0).astype(bf16)


def layer_major(rows, layers):
    size = rows * layers
    row = lax.broadcasted_iota(jnp.int32, (size, size), 0)
    col = lax.broadcasted_iota(jnp.int32, (size, size), 1)
    return jnp.where(row % rows * layers + row // rows == col, 1.0, 0.0).astype(bf16)


def spread_active(active, layers):
    rows, lat_dev = active.shape
    wide = dot(active, pair_expander(lat_dev, layers))
    layer = lax.broadcasted_iota(jnp.int32, wide.shape, 1) % layers
    parts = [jnp.where(layer == l, wide, 0.0).astype(bf16) for l in range(layers)]
    return jnp.concatenate(parts, axis=0)


def gather_kernel_body(n, src, buf, own_block, sems, me, send_to):
    chips = n // 2
    chip, core = me // 2, me % 2
    partner = me + 1 - 2 * core
    send, recv, fsend, frecv = sems

    def put(src_ref, index, ssem, rsem, dev):
        return pltpu.make_async_remote_copy(
            src_ref=src_ref, dst_ref=buf.at[index], send_sem=ssem, recv_sem=rsem,
            device_id={"lat": dev}, device_id_type=pl.DeviceIdType.MESH)

    first = []
    for q in range(1, chips):
        dev = lax.rem(chip + q, chips) * 2 + core
        c = put(src, me, send.at[q], recv.at[q], dev)
        c.start()
        first.append(c)
    second = [put(src, me, fsend.at[0], frecv.at[0], partner)]
    second[0].start()
    for q in range(1, chips):
        first[q - 1].wait_recv()
        origin = lax.rem(chip - q + chips, chips) * 2 + core
        c = put(buf.at[origin], origin, fsend.at[q], frecv.at[q], partner)
        c.start()
        second.append(c)
    own_block()
    for c in second:
        c.wait_recv()
    return first + second


def forward_kernel(n, acts, enc_hbm, bias, dec_hbm, dbias,
                   xl_out, rl_out, own_out, before_out, inv_out, norm_out,
                   enc, dec, w2, xbuf, rbuf, wide, rsrc, pair_out, pair_in, sum_out, sum_in,
                   local_sem, ag_sem, rg_sem, pair_sem, sum_sem):
    me = lax.axis_index("lat")
    chips = n // 2
    chip, core = me // 2, me % 2
    partner = me + 1 - 2 * core
    tok_dev, layers, width = acts.shape
    lat_dev = dec.shape[0]
    rows = n * tok_dev
    block = tok_dev * layers

    enc_copy = pltpu.make_async_copy(enc_hbm, enc, local_sem.at[0])
    dec_copy = pltpu.make_async_copy(dec_hbm, dec, local_sem.at[1])
    enc_copy.start()
    dec_copy.start()
    barrier = pltpu.get_barrier_semaphore()
    for q in range(1, chips):
        dev = lax.rem(chip + q, chips) * 2 + core
        pl.semaphore_signal(barrier, inc=1, device_id={"lat": dev}, device_id_type=pl.DeviceIdType.MESH)
    pl.semaphore_signal(barrier, inc=1, device_id={"lat": partner}, device_id_type=pl.DeviceIdType.MESH)
    pl.semaphore_wait(barrier, chips)

    def weight_work():
        xbuf[me] = acts[...]
        dec_copy.wait()
        square = jnp.zeros((lat_dev * layers, 128), f32)
        for c in range(0, width, 512):
            piece = dec[:, :, c:c + 512].reshape(lat_dev * layers, 512)
            w2[:, c:c + 512] = piece
            p = piece.astype(f32)
            p = p * p
            for k in range(4):
                square = square + p[:, k * 128:(k + 1) * 128]
        total = jnp.sum(square, axis=1, keepdims=True) + 1.0
        inv_out[...] = lax.rsqrt(total)
        norm = jnp.broadcast_to(jnp.sqrt(total), (lat_dev * layers, 128))
        norm_out[...] = jnp.transpose(norm)[:8, :]
        enc_copy.wait()

    started = gather_kernel_body(n, acts, xbuf, weight_work, [ag_sem.at[i] for i in range(4)], me, None)

    order_rows = layer_major(rows, layers)
    before = bias[...].reshape(1, lat_dev)
    for c in range(0, width, 512):
        piece = dot(order_rows, xbuf[:, :, :, c:c + 512].reshape(rows * layers, 512)).astype(bf16)
        xl_out[:, c:c + 512] = piece
        for l in range(layers):
            before = before + dot(piece[l * rows:(l + 1) * rows, :], enc[l, c:c + 512, :])
    before_out[...] = before
    active = jnp.maximum(before, 0.0).astype(bf16)
    spread = dot(order_rows, spread_active(active, layers), 0, 0).astype(bf16)
    for c in range(0, width, 512):
        wide[:, c:c + 512] = dot(spread, w2[:, c:c + 512])

    def chunk(dev):
        return wide[pl.ds(pl.multiple_of(dev * block, block), block), :]

    order = list(range(1, chips)) + [0]
    pairs = {}
    for q in order:
        k = lax.rem(chip + q, chips)
        pair_out[q] = chunk(k * 2 + 1 - core).astype(bf16)
        c = pltpu.make_async_remote_copy(
            src_ref=pair_out.at[q], dst_ref=pair_in.at[q], send_sem=pair_sem.at[0, q], recv_sem=pair_sem.at[1, q],
            device_id={"lat": partner}, device_id_type=pl.DeviceIdType.MESH)
        c.start()
        pairs[q] = c
    sums = []
    for q in order:
        k = lax.rem(chip + q, chips)
        pairs[q].wait_recv()
        both = chunk(k * 2 + core) + pair_in[q].astype(f32)
        if q == 0:
            total = both
        else:
            sum_out[q] = both.astype(bf16)
            c = pltpu.make_async_remote_copy(
                src_ref=sum_out.at[q], dst_ref=sum_in.at[q], send_sem=sum_sem.at[0, q], recv_sem=sum_sem.at[1, q],
                device_id={"lat": k * 2 + core}, device_id_type=pl.DeviceIdType.MESH)
            c.start()
            sums.append(c)
    layer = lax.broadcasted_iota(jnp.int32, (block, width), 0) % layers
    shift = jnp.zeros((block, width), f32)
    for l in range(layers):
        shift = jnp.where(layer == l, dbias[l:l + 1, :], shift)
    total = total + shift - acts[...].reshape(block, width).astype(f32)
    for q in range(1, chips):
        sums[q - 1].wait_recv()
        total = total + sum_in[q].astype(f32)
    residual = total.astype(bf16)
    rsrc[...] = residual
    own_out[...] = residual

    def own_residual():
        rbuf[me] = residual

    started += gather_kernel_body(n, rsrc, rbuf, own_residual, [rg_sem.at[i] for i in range(4)], me, None)
    for c in range(0, width, 512):
        piece = rbuf[:, :, c:c + 512].astype(f32).reshape(rows * layers, 512).astype(bf16)
        rl_out[:, c:c + 512] = dot(order_rows, piece).astype(bf16)
    for c in started + list(pairs.values()) + sums:
        c.wait_send()


def backward_kernel(xl, rl, own, before, inv, norm, dec, residual, genc, gencb, gdec, gdecb):
    layers, width, lat_dev = genc.shape
    rows = before.shape[0]
    factor = 2.0 / rows
    step = 512
    residual[...] = own[...].reshape(residual.shape)
    back = jnp.zeros((rows * layers, lat_dev * layers), f32)
    for c in range(0, width, step):
        back = back + dot(rl[:, c:c + step], dec[:, :, c:c + step].reshape(lat_dev * layers, step), 1, 1)
    layer = lax.broadcasted_iota(jnp.int32, (rows, lat_dev * layers), 1) % layers
    value = jnp.zeros((rows, lat_dev * layers), f32)
    for l in range(layers):
        value = jnp.where(layer == l, back[l * rows:(l + 1) * rows, :], value)
    value = factor * value + (sparsity_weight / rows) * norm[0:1, :]
    high = value.astype(bf16)
    low = (value - high.astype(f32)).astype(bf16)
    expand = pair_expander(lat_dev, layers)
    grad_act = dot(high, expand, 1, 1) + dot(low, expand, 1, 1)
    pre = before[...]
    grad_before = jnp.where(pre > 0.0, grad_act, 0.0).astype(bf16)
    gencb[...] = jnp.sum(grad_before.astype(f32), axis=0, keepdims=True)
    for l in range(layers):
        for c in range(0, width, step):
            genc[l, c:c + step, :] = dot(xl[l * rows:(l + 1) * rows, c:c + step], grad_before, 0, 0).astype(bf16)
    spread = spread_active(jnp.maximum(pre, 0.0).astype(bf16), layers)
    act_sum = dot(spread, jnp.ones((rows * layers, 128), bf16), 0, 0)[:, :1]
    scale = (sparsity_weight / rows) * act_sum * inv[...]
    for c in range(0, width, step):
        wide = dec[:, :, c:c + step].reshape(lat_dev * layers, step).astype(f32)
        out = factor * dot(spread, rl[:, c:c + step], 0, 0) + scale * wide
        gdec[:, :, c:c + step] = out.astype(bf16).reshape(lat_dev, layers, step)
    for l in range(layers):
        gdecb[l:l + 1, :] = factor * jnp.sum(rl[l * rows:(l + 1) * rows, :].astype(f32), axis=0, keepdims=True)


def body(n, acts, enc_weight, enc_bias, dec_weight, dec_bias):
    tok_dev, layers, width = acts.shape
    lat_dev = enc_weight.shape[2]
    rows, block, chips = n * tok_dev, tok_dev * layers, n // 2
    vmem = pl.BlockSpec(memory_space=pltpu.VMEM)
    hbm = pl.BlockSpec(memory_space=pl.ANY)
    shape = jax.ShapeDtypeStruct
    dma = pltpu.SemaphoreType.DMA
    xl, rl, own, before, inv, norm = pl.pallas_call(
        functools.partial(forward_kernel, n),
        out_shape=(
            shape((rows * layers, width), bf16),
            shape((rows * layers, width), bf16),
            shape((block, width), bf16),
            shape((rows, lat_dev), f32),
            shape((lat_dev * layers, 1), f32),
            shape((8, lat_dev * layers), f32),
        ),
        in_specs=[vmem, hbm, vmem, hbm, vmem],
        out_specs=(vmem,) * 6,
        scratch_shapes=[
            pltpu.VMEM(enc_weight.shape, bf16),
            pltpu.VMEM(dec_weight.shape, bf16),
            pltpu.VMEM((lat_dev * layers, width), bf16),
            pltpu.VMEM((n, tok_dev, layers, width), bf16),
            pltpu.VMEM((n, block, width), bf16),
            pltpu.VMEM((rows * layers, width), f32),
            pltpu.VMEM((block, width), bf16),
            pltpu.VMEM((chips, block, width), bf16),
            pltpu.VMEM((chips, block, width), bf16),
            pltpu.VMEM((chips, block, width), bf16),
            pltpu.VMEM((chips, block, width), bf16),
            dma((2,)),
            dma((4, chips)),
            dma((4, chips)),
            dma((2, chips)),
            dma((2, chips)),
        ],
        compiler_params=pltpu.CompilerParams(
            collective_id=0, has_side_effects=True, vmem_limit_bytes=56 * 1024 * 1024),
        name="forward",
    )(acts, enc_weight, enc_bias.reshape(1, lat_dev), dec_weight, dec_bias)
    residual, genc, gencb, gdec, gdecb = pl.pallas_call(
        backward_kernel,
        out_shape=(
            shape(acts.shape, bf16),
            shape(enc_weight.shape, bf16),
            shape((1, lat_dev), f32),
            shape(dec_weight.shape, bf16),
            shape(dec_bias.shape, f32),
        ),
        in_specs=[vmem] * 7,
        out_specs=(vmem,) * 5,
        compiler_params=pltpu.CompilerParams(vmem_limit_bytes=56 * 1024 * 1024),
        name="backward",
    )(xl, rl, own, before, inv, norm, dec_weight)
    return residual, genc, gencb.reshape(lat_dev), gdec, gdecb


def solution(mesh):
    specs = (
        P(("grp", "lat"), None, None),
        P("grp", None, "lat"),
        P(("grp", "lat")),
        P("lat", "grp", None),
        P("grp", None),
    )
    return jax.shard_map(
        functools.partial(body, mesh.shape["lat"]),
        mesh=mesh, in_specs=specs, out_specs=specs, check_vma=False,
    )
```
